1024 devices in a mesh: blk: 16 (over z_hi, x, core), group: 64 (over y, z_lo).
Axes of the slice: x: 4, y: 4, z: 32 (z_hi: 2, z_lo: 16; z = z_hi * 16 + z_lo), core: 2. Of those that a mesh axis runs over, the one named last changes fastest.
Arguments:
- queries: bfloat16 [64, 2048, 2048], P('group', 'blk'), may hold values from -300 to 300
- normed: bfloat16 [64, 2048, 2048], P('group', 'blk'), may hold values from -6 to 6
- key_weight_copies: bfloat16 [64, 2048, 512], P('group', 'blk'), may hold values from -0.125 to 0.125
- value_weight_copies: bfloat16 [64, 2048, 512], P('group', 'blk'), may hold values from -0.125 to 0.125
- owner: int32 [16], replicated, may hold values from 0 to 63
Outputs:
- cache_keys: bfloat16 [64, 2048, 512], P('group', 'blk')
- cache_values: bfloat16 [64, 2048, 512], P('group', 'blk')
- attended: bfloat16 [64, 2048, 2048], P('group', 'blk')
The draws below stay inside these ranges and needn't reach their ends.
Inputs may be any that keep to these rules, and one draw needn't show every extreme that they name: `owner`: learner group index of each block of projection rows, below the number of actor groups.
All inputs are finite; a program needn't handle non-finite values.
Results may differ from the reference program's by a relative error of at most 0.011.
Values may be sent and summed in bfloat16 or wider, within the bound.
No kernel may reach another device: no remote copies, remote signals or barrier semaphores. Data moves between devices by JAX's collectives and lax.ppermute only.
A program may use at most 64 MiB of HBM per device.

```python
import math
import jax
import jax.numpy as jnp
from jax import lax

INPUT_FEATURES = 2048
QUERY_HEADS = 16
KEY_VALUE_HEADS = 4
HEAD_SIZE = 128
PROMPT_TOKENS = 2048
ACTOR_GROUPS = 64
N_BLK = 16
N_GROUP = 64


def draw_queries(key, part):
    base_draw = jax.random.normal(jax.random.fold_in(key, 11), (ACTOR_GROUPS, PROMPT_TOKENS, QUERY_HEADS * HEAD_SIZE), jnp.float32)
    return jnp.clip(base_draw, -6.0, 6.0).astype(jnp.bfloat16)


def place_ends(entries, own_key, least, largest):
    extent = entries.shape
    spot = [jax.random.randint(jax.random.fold_in(own_key, axis), (), 0, extent[axis]) for axis in range(len(extent))]
    entries = entries.at[tuple(spot)].set(least)
    longest = extent.index(max(extent))
    spot[longest] = (spot[longest] + 1) % extent[longest]
    return entries.at[tuple(spot)].set(largest)


def level_of(stream_key, extent, shards, smallest, top_value):
    factor_of, own = 1.0, jax.random.fold_in(stream_key, 6)
    for position, blocks in shards:
        draws = jnp.exp(jax.random.uniform(jax.random.fold_in(own, position), (blocks,), jnp.float32, smallest / len(shards), top_value / len(shards)))
        factor_of = factor_of * jnp.repeat(draws, extent[position] // blocks).reshape([-1 if axis == position else 1 for axis in range(len(extent))])
    return factor_of


def scatter_about(stream_key, shape, width, limit, cuts=(), kind=jnp.bfloat16):
    factor_of = level_of(stream_key, shape, cuts, -0.22, 0.18) if cuts else 1.0
    result = jax.random.normal(stream_key, shape, jnp.float32) * width * factor_of
    return jnp.minimum(jnp.maximum(result, -limit), limit).astype(kind)


def setup_inputs(seed: int = 0) -> dict:
    seeds = jax.random.split(jax.random.key(seed), 6)
    return {
        "queries": draw_queries(jax.random.fold_in(seeds[5], 71), 0),
        "normed": scatter_about(seeds[1], (ACTOR_GROUPS, PROMPT_TOKENS, INPUT_FEATURES), 1.0, 6.0, ((0, 64), (1, 16))),
        "key_weight_copies": scatter_about(seeds[2], (ACTOR_GROUPS, INPUT_FEATURES, KEY_VALUE_HEADS * HEAD_SIZE), INPUT_FEATURES ** -0.5, 0.125, ((0, 64), (1, 16))),
        "value_weight_copies": scatter_about(seeds[3], (ACTOR_GROUPS, INPUT_FEATURES, KEY_VALUE_HEADS * HEAD_SIZE), INPUT_FEATURES ** -0.5, 0.125, ((0, 64), (1, 16))),
        "owner": place_ends(jax.random.randint(seeds[4], (N_BLK,), 0, N_GROUP), jax.random.fold_in(seeds[4], 1), 0, N_GROUP - 1).astype(jnp.int32),
    }


def rotate(unshaped_rows, positions):
    half_dim = HEAD_SIZE // 2
    inverse_freq = jnp.exp(jnp.arange(half_dim).astype(jnp.float32) * (-2.0 * math.log(500000.0) / HEAD_SIZE))
    angles = positions.astype(jnp.float32)[:, None] * inverse_freq[None, :]
    cos_table = jnp.cos(angles)[:, None, :]
    sin_table = jnp.sin(angles)[:, None, :]
    reshaped_rows = unshaped_rows.reshape(unshaped_rows.shape[0], KEY_VALUE_HEADS, HEAD_SIZE)
    first_half = reshaped_rows[..., :half_dim]
    second_half = reshaped_rows[..., half_dim:]
    transposed_rows = jnp.concatenate([first_half * cos_table - second_half * sin_table, second_half * cos_table + first_half * sin_table], axis=-1)
    return transposed_rows.reshape(unshaped_rows.shape[0], KEY_VALUE_HEADS * HEAD_SIZE)


def pick_rows(copies, owner):
    block_rows = INPUT_FEATURES // N_BLK
    blocked = copies.reshape(ACTOR_GROUPS, N_BLK, block_rows, copies.shape[2])
    chosen = blocked[owner.astype(jnp.int32), jnp.arange(N_BLK, dtype=jnp.int32)]
    return chosen.reshape(INPUT_FEATURES, copies.shape[2])


def reference(queries, normed, key_weight_copies, value_weight_copies, owner):
    key_proj = pick_rows(key_weight_copies, owner)
    value_proj = pick_rows(value_weight_copies, owner)
    positions = jnp.arange(PROMPT_TOKENS)
    allowed = positions[None, :] <= positions[:, None]

    def per_actor(actor_pair):
        projected_query_rows, input_rows = actor_pair
        layer_key_cache = rotate(jnp.dot(input_rows, key_proj, preferred_element_type=jnp.float32), positions).astype(jnp.bfloat16)
        value_rows = jnp.dot(input_rows, value_proj, preferred_element_type=jnp.float32).astype(jnp.bfloat16)
        query_head_grid = projected_query_rows.reshape(PROMPT_TOKENS, KEY_VALUE_HEADS, QUERY_HEADS // KEY_VALUE_HEADS, HEAD_SIZE).astype(jnp.float32)
        full_score_matrix = jnp.einsum('lewc,jec->ewlj', query_head_grid, layer_key_cache.reshape(PROMPT_TOKENS, KEY_VALUE_HEADS, HEAD_SIZE).astype(jnp.float32)) * (HEAD_SIZE ** -0.5)
        full_score_matrix = jnp.where(allowed, full_score_matrix, -jnp.inf)
        row_max = jnp.max(full_score_matrix, axis=-1, keepdims=True)
        full_probabilities = jnp.exp(full_score_matrix - row_max)
        row_total = jnp.sum(full_probabilities, axis=-1)
        weighted_values = jnp.einsum('lxbp,plj->lxbj', full_probabilities.astype(jnp.bfloat16).astype(jnp.float32), value_rows.reshape(PROMPT_TOKENS, KEY_VALUE_HEADS, HEAD_SIZE).astype(jnp.float32))
        mixed_out = weighted_values / row_total[..., None]
        attended = mixed_out.transpose(2, 0, 1, 3).reshape(PROMPT_TOKENS, QUERY_HEADS * HEAD_SIZE).astype(jnp.bfloat16)
        return layer_key_cache, value_rows, attended

    cache_keys, cache_values, attended = lax.map(per_actor, (queries, normed))
    return cache_keys, cache_values, attended
```

```python
import math

import jax
import jax.numpy as jnp
from jax import lax
from jax.experimental import pallas as pl
from jax.experimental.pallas import tpu as pltpu
from jax.sharding import Mesh
from jax.sharding import PartitionSpec as P

HEAD = 128
SCALE = HEAD ** (-0.5)
NEG = -1e30
QB = 256
AXES = ("zh", "x", "c", "y", "zf", "zn")
RING = ("zh", "zf", "zn")
VM = pl.BlockSpec(memory_space=pltpu.VMEM)
SM = pl.BlockSpec(memory_space=pltpu.SMEM)
NT = (((1,), (1,)), ((), ()))


def exchange(x, axes):
    return lax.all_to_all(x, axes, 0, 0, tiled=True)


def spread(x, axes, n):
    return exchange(jnp.broadcast_to(x[None], (n,) + x.shape), axes)


def pick(x, index):
    n = index.shape[0]

    def kernel(i_ref, x_ref, o_ref):
        for k in range(n):
            o_ref[k] = x_ref[i_ref[k]]

    return pl.pallas_call(
        kernel,
        out_shape=jax.ShapeDtypeStruct((n,) + x.shape[1:], x.dtype),
        in_specs=[SM, VM],
        out_specs=VM,
        name="pick",
    )(index, x)


def tables(zh, c):
    half = HEAD // 2
    freq = jnp.exp(
        jnp.arange(half).astype(jnp.float32) * (-2.0 * math.log(500000.0) / HEAD)
    )
    t = zh * 1024 + jnp.arange(1024, dtype=jnp.int32)
    angles = t.astype(jnp.float32)[:, None] * freq[None, :]
    cos, sin = jnp.cos(angles), jnp.sin(angles)
    cos = jnp.concatenate([cos, cos], axis=1)
    sin = jnp.concatenate([-sin, sin], axis=1)
    is_key = c == 0
    return jnp.where(is_key, cos, 1.0), jnp.where(is_key, sin, 0.0)


def project(place, mine, other, w, cos, sin):
    def kernel(p_ref, a0, a1, a2, a3, b_ref, w_ref, cos_ref, sin_ref, o_ref):
        for k in range(8):
            s = k % 4
            piece = (a0, a1, a2, a3)[s][...] if k < 4 else b_ref[s]
            raw = jnp.dot(piece, w_ref[...], preferred_element_type=jnp.float32)
            rows = pl.ds(pl.multiple_of(p_ref[k] * 128, 128), 128)
            turned = raw * cos_ref[rows, :] + pltpu.roll(raw, 64, 1) * sin_ref[rows, :]
            o_ref[rows, :] = turned.astype(jnp.bfloat16)

    return pl.pallas_call(
        kernel,
        out_shape=jax.ShapeDtypeStruct((1024, HEAD), jnp.bfloat16),
        in_specs=[SM] + [VM] * 8,
        out_specs=VM,
        name="project",
    )(place, *mine, other, w, cos, sin)


def attend_own(q, k, v):
    def kernel(q_ref, k_ref, v_ref, acc_ref, m_ref, l_ref):
        for h in range(2):
            col = pl.ds(h * HEAD, HEAD)
            for i in range(1024 // QB):
                rows = pl.ds(i * QB, QB)
                n = (i + 1) * QB
                s = lax.dot_general(
                    q_ref[rows, col], k_ref[:n, :], NT, preferred_element_type=jnp.float32
                )
                r = lax.broadcasted_iota(jnp.int32, (QB, n), 0) + i * QB
                t = lax.broadcasted_iota(jnp.int32, (QB, n), 1)
                s = jnp.where(t <= r, s, NEG)
                m = jnp.max(s, axis=1, keepdims=True)
                p = jnp.exp((s - m) * SCALE)
                m_ref[h, rows, :] = m
                l_ref[h, rows, :] = jnp.sum(p, axis=1, keepdims=True)
                acc_ref[rows, col] = jnp.dot(
                    p.astype(jnp.bfloat16), v_ref[:n, :], preferred_element_type=jnp.float32
                )

    stat = jax.ShapeDtypeStruct((2, 1024, 1), jnp.float32)
    return pl.pallas_call(
        kernel,
        out_shape=(jax.ShapeDtypeStruct((1024, 256), jnp.float32), stat, stat),
        in_specs=[VM] * 3,
        out_specs=(VM,) * 3,
        name="attend_own",
    )(q, k, v)


def attend_rest(zh, q, k, v, acc, m, l):
    def kernel(z_ref, q_ref, k_ref, v_ref, acc_ref, m_ref, l_ref, o_ref):
        @pl.when(z_ref[0] == 0)
        def _():
            for h in range(2):
                col = pl.ds(h * HEAD, HEAD)
                o_ref[:, col] = (acc_ref[:, col] / l_ref[h]).astype(jnp.bfloat16)

        @pl.when(z_ref[0] != 0)
        def _():
            for h in range(2):
                col = pl.ds(h * HEAD, HEAD)
                for i in range(1024 // QB):
                    rows = pl.ds(i * QB, QB)
                    s = lax.dot_general(
                        q_ref[rows, col], k_ref[...], NT, preferred_element_type=jnp.float32
                    )
                    m0 = m_ref[h, rows, :]
                    m1 = jnp.maximum(m0, jnp.max(s, axis=1, keepdims=True))
                    fade = jnp.exp((m0 - m1) * SCALE)
                    p = jnp.exp((s - m1) * SCALE)
                    total = l_ref[h, rows, :] * fade + jnp.sum(p, axis=1, keepdims=True)
                    out = acc_ref[rows, col] * fade + jnp.dot(
                        p.astype(jnp.bfloat16), v_ref[...], preferred_element_type=jnp.float32
                    )
                    o_ref[rows, col] = (out / total).astype(jnp.bfloat16)

    return pl.pallas_call(
        kernel,
        out_shape=jax.ShapeDtypeStruct((1024, 256), jnp.bfloat16),
        in_specs=[SM] + [VM] * 6,
        out_specs=VM,
        name="attend_rest",
    )(zh.reshape(1), q, k, v, acc, m, l)


def swap_cores(x):
    return lax.ppermute(x, "c", [(0, 1), (1, 0)])


def body(queries, normed, key_weight_copies, value_weight_copies, owner):
    zh, x, c = lax.axis_index("zh"), lax.axis_index("x"), lax.axis_index("c")
    z_lo = lax.axis_index(("zf", "zn"))
    own_y, own_zf, own_zn = owner // 16, (owner // 4) % 4, owner % 4
    block8 = jnp.arange(8, dtype=jnp.int32)
    n = normed[0]

    w = jnp.stack([key_weight_copies[0], value_weight_copies[0]])
    w = w.reshape(2, 16, 8, 4, HEAD).transpose(3, 0, 1, 2, 4).reshape(128, 8, HEAD)
    w = exchange(w, ("x", "c", "y", "zn"))
    here = lax.dynamic_slice_in_dim(own_y * 4 + own_zn, zh * 8, 8)
    w = pick(w, block8 * 16 + here)

    rows = [n] + [lax.ppermute(n, "x", [(i, (i + s) % 4) for i in range(4)]) for s in (1, 2, 3)]

    w = spread(w, ("zh", "zf"), 8)
    block16 = jnp.arange(16, dtype=jnp.int32)
    w = pick(w.reshape(64, 8, HEAD), ((block16 // 8) * 4 + own_zf) * 8 + block16 % 8)

    other = swap_cores(jnp.stack(rows))

    w = spread(w, ("y", "zn"), 16).reshape(16, 16, 8, HEAD)
    w = w.transpose(1, 0, 2, 3).reshape(2048, HEAD)

    chip = (x - jnp.arange(4, dtype=jnp.int32)) % 4
    place = jnp.concatenate([chip * 2 + c, chip * 2 + 1 - c])
    cos, sin = tables(zh, c)
    kv = project(place, rows, other, w, cos, sin)

    up = lax.ppermute(kv, RING, [(i, i + 15) for i in range(8, 16)])
    down = lax.ppermute(kv, RING, [(i, i + 17) for i in range(8)])

    partner = swap_cores(kv)
    keys, values = jnp.where(c == 0, kv, partner), jnp.where(c == 0, partner, kv)
    q = queries[0].reshape(128, 8, 256).transpose(1, 0, 2)
    q = exchange(q, ("x", "c")).reshape(1024, 256)
    acc, m, l = attend_own(q, keys, values)
    cache = exchange(kv.reshape(8, 128, HEAD), ("x", "c")).reshape(4, 2, 128, HEAD)
    cache_keys = cache[:, 0].transpose(1, 0, 2).reshape(1, 128, 512)
    cache_values = cache[:, 1].transpose(1, 0, 2).reshape(1, 128, 512)

    up = lax.ppermute(up, RING, [(i, i + 1) for i in range(23, 31)])
    down = lax.ppermute(down, RING, [(i, i - 1) for i in range(17, 25)])
    first = jnp.where(z_lo >= 8, up, down)
    partner = swap_cores(first)
    keys, values = jnp.where(c == 0, first, partner), jnp.where(c == 0, partner, first)
    out = attend_rest(zh, q, keys, values, acc, m, l)
    out = exchange(out.reshape(8, 128, 256), ("x", "c"))
    attended = out.transpose(1, 0, 2).reshape(1, 128, 2048)
    return cache_keys, cache_values, attended


def solution(mesh):
    torus = Mesh(mesh.devices.reshape(2, 4, 2, 4, 4, 4), AXES)
    spec = P(("y", "zf", "zn"), ("zh", "x", "c"), None)
    return jax.shard_map(
        body,
        mesh=torus,
        in_specs=(spec, spec, spec, spec, P()),
        out_specs=(spec, spec, spec),
        check_vma=False,
    )
```

```python
import math

import jax
import jax.numpy as jnp
from jax import lax
from jax.experimental import pallas as pl
from jax.experimental.pallas import tpu as pltpu
from jax.sharding import Mesh
from jax.sharding import PartitionSpec as P


HEAD = 128
SCALE = HEAD ** (-0.5)
NEG = -1e30
QB = 256
CHUNKS = 2
STEP = 1024 // CHUNKS
AXES = ("zh", "x", "c", "y", "zf", "zn")
RING = ("zh", "zf", "zn")
VM = pl.BlockSpec(memory_space=pltpu.VMEM)
SM = pl.BlockSpec(memory_space=pltpu.SMEM)
NT = (((1,), (1,)), ((), ()))
STATE = (
    jax.ShapeDtypeStruct((1024, 256), jnp.float32),
    jax.ShapeDtypeStruct((1024, 4), jnp.float32),
)


def exchange(x, axes):
    return lax.all_to_all(x, axes, 0, 0, tiled=True)


def spread(x, axes, n):
    return exchange(jnp.broadcast_to(x[None], (n,) + x.shape), axes)


def pick(x, index):
    n = index.shape[0]

    def kernel(i_ref, x_ref, o_ref):
        for k in range(n):
            o_ref[k] = x_ref[i_ref[k]]

    return pl.pallas_call(
        kernel,
        out_shape=jax.ShapeDtypeStruct((n,) + x.shape[1:], x.dtype),
        in_specs=[SM, VM],
        out_specs=VM,
        name="pick",
    )(index, x)


def tables(zh, c):
    half = HEAD // 2
    freq = jnp.exp(
        jnp.arange(half).astype(jnp.float32) * (-2.0 * math.log(500000.0) / HEAD)
    )
    t = zh * 1024 + jnp.arange(1024, dtype=jnp.int32)
    angles = t.astype(jnp.float32)[:, None] * freq[None, :]
    cos, sin = jnp.cos(angles), jnp.sin(angles)
    cos = jnp.concatenate([cos, cos], axis=1)
    sin = jnp.concatenate([-sin, sin], axis=1)
    is_key = c == 0
    return jnp.where(is_key, cos, 1.0), jnp.where(is_key, sin, 0.0)


def project(place, mine, other, w, cos, sin):
    def kernel(p_ref, a0, a1, a2, a3, b_ref, w_ref, cos_ref, sin_ref, o_ref):
        for k in range(8):
            s = k % 4
            piece = (a0, a1, a2, a3)[s][...] if k < 4 else b_ref[s]
            raw = jnp.dot(piece, w_ref[...], preferred_element_type=jnp.float32)
            rows = pl.ds(pl.multiple_of(p_ref[k] * 128, 128), 128)
            turned = raw * cos_ref[rows, :] + pltpu.roll(raw, 64, 1) * sin_ref[rows, :]
            o_ref[rows, :] = turned.astype(jnp.bfloat16)

    return pl.pallas_call(
        kernel,
        out_shape=jax.ShapeDtypeStruct((1024, HEAD), jnp.bfloat16),
        in_specs=[SM] + [VM] * 8,
        out_specs=VM,
        name="project",
    )(place, *mine, other, w, cos, sin)


def attend_own(q, k, v):
    def kernel(q_ref, k_ref, v_ref, acc_ref, st_ref):
        for i in range(1024 // QB):
            rows = pl.ds(i * QB, QB)
            n = (i + 1) * QB
            r = lax.broadcasted_iota(jnp.int32, (QB, n), 0) + i * QB
            t = lax.broadcasted_iota(jnp.int32, (QB, n), 1)
            tops, totals = [], []
            for h in range(2):
                col = pl.ds(h * HEAD, HEAD)
                s = lax.dot_general(
                    q_ref[rows, col], k_ref[:n, :], NT, preferred_element_type=jnp.float32
                )
                s = jnp.where(t <= r, s, NEG)
                m = jnp.max(s, axis=1, keepdims=True)
                p = jnp.exp((s - m) * SCALE)
                tops.append(m)
                totals.append(jnp.sum(p, axis=1, keepdims=True))
                acc_ref[rows, col] = jnp.dot(
                    p.astype(jnp.bfloat16), v_ref[:n, :], preferred_element_type=jnp.float32
                )
            st_ref[rows, :] = jnp.concatenate(tops + totals, axis=1)

    return pl.pallas_call(
        kernel,
        out_shape=STATE,
        in_specs=[VM] * 3,
        out_specs=(VM,) * 2,
        name="attend_own",
    )(q, k, v)


def attend_more(zh, q, k, v, acc, st, last):
    n = k.shape[0]

    def kernel(z_ref, q_ref, k_ref, v_ref, acc_ref, st_ref, *outs):
        def leave(col, acc, total):
            if last:
                outs[0][:, col] = (acc / total).astype(jnp.bfloat16)
            else:
                outs[0][:, col] = acc

        @pl.when(z_ref[0] == 0)
        def _():
            for h in range(2):
                col = pl.ds(h * HEAD, HEAD)
                leave(col, acc_ref[:, col], st_ref[:, 2 + h : 3 + h])
            if not last:
                outs[1][...] = st_ref[...]

        @pl.when(z_ref[0] != 0)
        def _():
            tops, totals = [], []
            for h in range(2):
                col = pl.ds(h * HEAD, HEAD)
                s = lax.dot_general(
                    q_ref[:, col], k_ref[...], NT, preferred_element_type=jnp.float32
                )
                m0 = st_ref[:, h : h + 1]
                m1 = jnp.maximum(m0, jnp.max(s, axis=1, keepdims=True))
                fade = jnp.exp((m0 - m1) * SCALE)
                p = jnp.exp((s - m1) * SCALE)
                total = st_ref[:, 2 + h : 3 + h] * fade + jnp.sum(p, axis=1, keepdims=True)
                out = acc_ref[:, col] * fade + jnp.dot(
                    p.astype(jnp.bfloat16), v_ref[...], preferred_element_type=jnp.float32
                )
                leave(col, out, total)
                tops.append(m1)
                totals.append(total)
            if not last:
                outs[1][...] = jnp.concatenate(tops + totals, axis=1)

    row = lambda width: pl.BlockSpec((QB, width), lambda i: (i, 0))
    whole = pl.BlockSpec((n, HEAD), lambda i: (0, 0))
    out = jax.ShapeDtypeStruct((1024, 256), jnp.bfloat16)
    return pl.pallas_call(
        kernel,
        grid=(1024 // QB,),
        out_shape=out if last else STATE,
        in_specs=[SM, row(256), whole, whole, row(256), row(4)],
        out_specs=row(256) if last else (row(256), row(4)),
        name="attend_more",
    )(zh.reshape(1), q, k, v, acc, st)


def swap_cores(x):
    return lax.ppermute(x, "c", [(0, 1), (1, 0)])


def layer(queries, normed, key_weight_copies, value_weight_copies, owner):
    zh, x, c = lax.axis_index("zh"), lax.axis_index("x"), lax.axis_index("c")
    z_lo = lax.axis_index(("zf", "zn"))
    own_y, own_zf, own_zn = owner // 16, (owner // 4) % 4, owner % 4
    block8 = jnp.arange(8, dtype=jnp.int32)
    n = normed[0]

    w = jnp.stack([key_weight_copies[0], value_weight_copies[0]])
    w = w.reshape(2, 16, 8, 4, HEAD).transpose(3, 0, 1, 2, 4).reshape(128, 8, HEAD)
    w = exchange(w, ("x", "c", "y", "zn"))
    here = lax.dynamic_slice_in_dim(own_y * 4 + own_zn, zh * 8, 8)
    w = pick(w, block8 * 16 + here)

    rows = [n]
    for s in (1, 2, 3):
        rows.append(lax.ppermute(n, "x", [(i, (i + s) % 4) for i in range(4)]))

    w = spread(w, ("zh", "zf"), 8)
    block16 = jnp.arange(16, dtype=jnp.int32)
    w = pick(w.reshape(64, 8, HEAD), ((block16 // 8) * 4 + own_zf) * 8 + block16 % 8)

    other = swap_cores(jnp.stack(rows))

    w = spread(w, ("y", "zn"), 16).reshape(16, 16, 8, HEAD)
    w = w.transpose(1, 0, 2, 3).reshape(2048, HEAD)

    chip = (x - jnp.arange(4, dtype=jnp.int32)) % 4
    place = jnp.concatenate([chip * 2 + c, chip * 2 + 1 - c])
    cos, sin = tables(zh, c)
    kv = project(place, rows, other, w, cos, sin)

    ups, downs = [], []
    for k in range(CHUNKS):
        part = kv[k * STEP : (k + 1) * STEP]
        ups.append(lax.ppermute(part, RING, [(i, i + 15) for i in range(8, 16)]))
        downs.append(lax.ppermute(part, RING, [(i, i + 17) for i in range(8)]))

    partner = swap_cores(kv)
    keys, values = jnp.where(c == 0, kv, partner), jnp.where(c == 0, partner, kv)
    q = queries[0].reshape(128, 8, 256).transpose(1, 0, 2)
    q = exchange(q, ("x", "c")).reshape(1024, 256)
    state = attend_own(q, keys, values)
    cache = exchange(kv.reshape(8, 128, HEAD), ("x", "c")).reshape(4, 2, 128, HEAD)
    cache_keys = cache[:, 0].transpose(1, 0, 2).reshape(1, 128, 512)
    cache_values = cache[:, 1].transpose(1, 0, 2).reshape(1, 128, 512)

    ups[0], downs[0], state, cache_keys, cache_values = lax.optimization_barrier(
        (ups[0], downs[0], state, cache_keys, cache_values)
    )
    for k in range(CHUNKS):
        if k:
            ups[k], downs[k], state = lax.optimization_barrier((ups[k], downs[k], state))
        up = lax.ppermute(ups[k], RING, [(i, i + 1) for i in range(23, 31)])
        down = lax.ppermute(downs[k], RING, [(i, i - 1) for i in range(17, 25)])
        first = jnp.where(z_lo >= 8, up, down)
        partner = swap_cores(first)
        keys, values = jnp.where(c == 0, first, partner), jnp.where(c == 0, partner, first)
        state = attend_more(zh, q, keys, values, *state, k == CHUNKS - 1)
    out = exchange(state.reshape(8, 128, 256), ("x", "c"))
    attended = out.transpose(1, 0, 2).reshape(1, 128, 2048)
    return cache_keys, cache_values, attended


def solution(mesh):
    torus = Mesh(mesh.devices.reshape(2, 4, 2, 4, 4, 4), AXES)
    spec = P(("y", "zf", "zn"), ("zh", "x", "c"), None)
    return jax.shard_map(
        layer,
        mesh=torus,
        in_specs=(spec, spec, spec, spec, P()),
        out_specs=(spec, spec, spec),
        check_vma=False,
    )
```

```python
import math

import jax
import jax.numpy as jnp
from jax import lax
from jax.experimental import pallas as pl
from jax.experimental.pallas import tpu as pltpu
from jax.sharding import Mesh
from jax.sharding import PartitionSpec as P


HEAD = 128
SCALE = HEAD ** (-0.5)
NEG = -1e30
QB = 256
CHUNKS = 1
STEP = 1024 // CHUNKS
AXES = ("zh", "x", "c", "y", "zf", "zn")
RING = ("zh", "zf", "zn")
VM = pl.BlockSpec(memory_space=pltpu.VMEM)
SM = pl.BlockSpec(memory_space=pltpu.SMEM)
NT = (((1,), (1,)), ((), ()))
STATE = (
    jax.ShapeDtypeStruct((1024, 256), jnp.float32),
    jax.ShapeDtypeStruct((1024, 4), jnp.float32),
)


def exchange(x, axes):
    return lax.all_to_all(x, axes, 0, 0, tiled=True)


def pick_spread(x, index, copies, axes):
    n = index.shape[0]

    def kernel(i_ref, x_ref, o_ref):
        for k in range(n):
            piece = x_ref[i_ref[k]]
            for j in range(copies):
                o_ref[j, k] = piece

    many = pl.pallas_call(
        kernel,
        out_shape=jax.ShapeDtypeStruct((copies, n) + x.shape[1:], x.dtype),
        in_specs=[SM, VM],
        out_specs=VM,
        name="pick",
    )(index, x)
    return exchange(many, axes)


def tables(zh, c):
    half = HEAD // 2
    freq = jnp.exp(
        jnp.arange(half).astype(jnp.float32) * (-2.0 * math.log(500000.0) / HEAD)
    )
    t = zh * 1024 + jnp.arange(1024, dtype=jnp.int32)
    angles = t.astype(jnp.float32)[:, None] * freq[None, :]
    cos, sin = jnp.cos(angles), jnp.sin(angles)
    cos = jnp.concatenate([cos, cos], axis=1)
    sin = jnp.concatenate([-sin, sin], axis=1)
    is_key = c == 0
    return jnp.where(is_key, cos, 1.0), jnp.where(is_key, sin, 0.0)


def project(place, mine, other, w, cos, sin):
    def kernel(p_ref, a0, a1, a2, a3, b_ref, w_ref, cos_ref, sin_ref, o_ref, rows, wv, cv, sv, sems):
        pairs = [(w_ref, wv)]
        pairs += [(a, rows.at[0, pl.ds(128 * k, 128)]) for k, a in enumerate((a0, a1, a2, a3))]
        pairs += [(cos_ref, cv), (sin_ref, sv), (b_ref, rows.at[1])]
        copies = [pltpu.make_async_copy(s, d, sems.at[k]) for k, (s, d) in enumerate(pairs)]
        for copy in copies:
            copy.start()
        for copy in copies[:5]:
            copy.wait()
        for g in range(2):
            raw = jnp.dot(rows[g], wv[...], preferred_element_type=jnp.float32)
            for copy in copies[5:7] if g == 0 else []:
                copy.wait()
            for k in range(4):
                part = raw[128 * k : 128 * (k + 1)]
                to = pl.ds(pl.multiple_of(p_ref[4 * g + k] * 128, 128), 128)
                turned = part * cv[to, :] + pltpu.roll(part, 64, 1) * sv[to, :]
                o_ref[to, :] = turned.astype(jnp.bfloat16)
            if g == 0:
                copies[7].wait()

    return pl.pallas_call(
        kernel,
        out_shape=jax.ShapeDtypeStruct((1024, HEAD), jnp.bfloat16),
        in_specs=[SM] + [pl.BlockSpec(memory_space=pl.ANY)] * 8,
        out_specs=VM,
        scratch_shapes=[
            pltpu.VMEM((2, 512, 2048), jnp.bfloat16),
            pltpu.VMEM((2048, HEAD), jnp.bfloat16),
            pltpu.VMEM((1024, HEAD), jnp.float32),
            pltpu.VMEM((1024, HEAD), jnp.float32),
            pltpu.SemaphoreType.DMA((8,)),
        ],
        name="project",
    )(place, *mine, other, w, cos, sin)


def attend_own(q, k, v):
    def kernel(q_ref, k_ref, v_ref, acc_ref, st_ref):
        for i in range(1024 // QB):
            rows = pl.ds(i * QB, QB)
            n = (i + 1) * QB
            r = lax.broadcasted_iota(jnp.int32, (QB, n), 0) + i * QB
            t = lax.broadcasted_iota(jnp.int32, (QB, n), 1)
            tops, totals = [], []
            for h in range(2):
                col = pl.ds(h * HEAD, HEAD)
                s = lax.dot_general(
                    q_ref[rows, col], k_ref[:n, :], NT, preferred_element_type=jnp.float32
                )
                s = jnp.where(t <= r, s, NEG)
                m = jnp.max(s, axis=1, keepdims=True)
                p = jnp.exp((s - m) * SCALE)
                tops.append(m)
                totals.append(jnp.sum(p, axis=1, keepdims=True))
                acc_ref[rows, col] = jnp.dot(
                    p.astype(jnp.bfloat16), v_ref[:n, :], preferred_element_type=jnp.float32
                )
            st_ref[rows, :] = jnp.concatenate(tops + totals, axis=1)

    return pl.pallas_call(
        kernel,
        out_shape=STATE,
        in_specs=[VM] * 3,
        out_specs=(VM,) * 2,
        name="attend_own",
    )(q, k, v)


def attend_more(zh, q, k, v, acc, st, last):
    n = k.shape[0]

    def kernel(z_ref, q_ref, k_ref, v_ref, acc_ref, st_ref, *outs):
        def leave(col, acc, total):
            if last:
                outs[0][:, col] = (acc / total).astype(jnp.bfloat16)
            else:
                outs[0][:, col] = acc

        @pl.when(z_ref[0] == 0)
        def _():
            for h in range(2):
                col = pl.ds(h * HEAD, HEAD)
                leave(col, acc_ref[:, col], st_ref[:, 2 + h : 3 + h])
            if not last:
                outs[1][...] = st_ref[...]

        @pl.when(z_ref[0] != 0)
        def _():
            tops, totals = [], []
            for h in range(2):
                col = pl.ds(h * HEAD, HEAD)
                s = lax.dot_general(
                    q_ref[:, col], k_ref[...], NT, preferred_element_type=jnp.float32
                )
                m0 = st_ref[:, h : h + 1]
                m1 = jnp.maximum(m0, jnp.max(s, axis=1, keepdims=True))
                fade = jnp.exp((m0 - m1) * SCALE)
                p = jnp.exp((s - m1) * SCALE)
                total = st_ref[:, 2 + h : 3 + h] * fade + jnp.sum(p, axis=1, keepdims=True)
                out = acc_ref[:, col] * fade + jnp.dot(
                    p.astype(jnp.bfloat16), v_ref[...], preferred_element_type=jnp.float32
                )
                leave(col, out, total)
                tops.append(m1)
                totals.append(total)
            if not last:
                outs[1][...] = jnp.concatenate(tops + totals, axis=1)

    row = lambda width: pl.BlockSpec((QB, width), lambda i: (i, 0))
    whole = pl.BlockSpec((n, HEAD), lambda i: (0, 0))
    out = jax.ShapeDtypeStruct((1024, 256), jnp.bfloat16)
    return pl.pallas_call(
        kernel,
        grid=(1024 // QB,),
        out_shape=out if last else STATE,
        in_specs=[SM, row(256), whole, whole, row(256), row(4)],
        out_specs=row(256) if last else (row(256), row(4)),
        name="attend_more",
    )(zh.reshape(1), q, k, v, acc, st)


def swap_cores(x):
    return lax.ppermute(x, "c", [(0, 1), (1, 0)])


def layer(queries, normed, key_weight_copies, value_weight_copies, owner):
    zh, x, c = lax.axis_index("zh"), lax.axis_index("x"), lax.axis_index("c")
    z_lo = lax.axis_index(("zf", "zn"))
    own_y, own_zf, own_zn = owner // 16, (owner // 4) % 4, owner % 4
    block8 = jnp.arange(8, dtype=jnp.int32)
    n = normed[0]

    w = jnp.stack([key_weight_copies[0], value_weight_copies[0]])
    w = w.reshape(2, 16, 8, 4, HEAD).transpose(3, 0, 1, 2, 4).reshape(128, 8, HEAD)
    w = exchange(w, ("x", "c", "y", "zn"))
    here = lax.dynamic_slice_in_dim(own_y * 4 + own_zn, zh * 8, 8)
    rows = [n]
    for s in (1, 2, 3):
        rows.append(lax.ppermute(n, "x", [(i, (i + s) % 4) for i in range(4)]))

    w = pick_spread(w, block8 * 16 + here, 8, ("zh", "zf"))
    block16 = jnp.arange(16, dtype=jnp.int32)
    index = ((block16 // 8) * 4 + own_zf) * 8 + block16 % 8
    w = pick_spread(w.reshape(64, 8, HEAD), index, 16, ("y", "zn"))
    w = w.transpose(1, 0, 2, 3).reshape(2048, HEAD)

    other = swap_cores(jnp.concatenate(rows))

    chip = (x - jnp.arange(4, dtype=jnp.int32)) % 4
    place = jnp.concatenate([chip * 2 + c, chip * 2 + 1 - c])
    cos, sin = tables(zh, c)
    kv = project(place, rows, other, w, cos, sin)

    ups, downs = [], []
    for k in range(CHUNKS):
        part = kv[k * STEP : (k + 1) * STEP]
        ups.append(lax.ppermute(part, RING, [(i, i + 15) for i in range(8, 16)]))
        downs.append(lax.ppermute(part, RING, [(i, i + 17) for i in range(8)]))

    partner = swap_cores(kv)
    keys, values = jnp.where(c == 0, kv, partner), jnp.where(c == 0, partner, kv)
    q = queries[0].reshape(128, 8, 256).transpose(1, 0, 2)
    q = exchange(q, ("x", "c")).reshape(1024, 256)
    state = attend_own(q, keys, values)
    cache = exchange(kv.reshape(8, 128, HEAD), ("x", "c")).reshape(4, 2, 128, HEAD)
    cache_keys = cache[:, 0].transpose(1, 0, 2).reshape(1, 128, 512)
    cache_values = cache[:, 1].transpose(1, 0, 2).reshape(1, 128, 512)

    ups[0], downs[0], state, cache_keys, cache_values = lax.optimization_barrier(
        (ups[0], downs[0], state, cache_keys, cache_values)
    )
    for k in range(CHUNKS):
        if k:
            ups[k], downs[k], state = lax.optimization_barrier((ups[k], downs[k], state))
        up = lax.ppermute(ups[k], RING, [(i, i + 1) for i in range(23, 31)])
        down = lax.ppermute(downs[k], RING, [(i, i - 1) for i in range(17, 25)])
        first = jnp.where(z_lo >= 8, up, down)
        partner = swap_cores(first)
        keys, values = jnp.where(c == 0, first, partner), jnp.where(c == 0, partner, first)
        state = attend_more(zh, q, keys, values, *state, k == CHUNKS - 1)
    out = exchange(state.reshape(8, 128, 256), ("x", "c"))
    attended = out.transpose(1, 0, 2).reshape(1, 128, 2048)
    return cache_keys, cache_values, attended


def solution(mesh):
    torus = Mesh(mesh.devices.reshape(2, 4, 2, 4, 4, 4), AXES)
    spec = P(("y", "zf", "zn"), ("zh", "x", "c"), None)
    return jax.shard_map(
        layer,
        mesh=torus,
        in_specs=(spec, spec, spec, spec, P()),
        out_specs=(spec, spec, spec),
        check_vma=False,
    )
```

```python
import math

import jax
import jax.numpy as jnp
from jax import lax
from jax.experimental import pallas as pl
from jax.experimental.pallas import tpu as pltpu
from jax.sharding import Mesh
from jax.sharding import PartitionSpec as P


HEAD = 128
SCALE = HEAD ** (-0.5)
SCALE2 = SCALE * math.log2(math.e)
NEG = -1e30
QB = 256
AXES = ("zh", "x", "c", "y", "zf", "zn")
RING = ("zh", "zf", "zn")
VM = pl.BlockSpec(memory_space=pltpu.VMEM)
SM = pl.BlockSpec(memory_space=pltpu.SMEM)
NT = (((1,), (1,)), ((), ()))
STATE = (
    jax.ShapeDtypeStruct((1024, 256), jnp.float32),
    jax.ShapeDtypeStruct((1024, 4), jnp.float32),
)


def exchange(x, axes):
    return lax.all_to_all(x, axes, 0, 0, tiled=True)


def pick_spread(x, index, copies, axes):
    n = index.shape[0]

    def kernel(i_ref, x_ref, o_ref):
        for k in range(n):
            piece = x_ref[i_ref[k]]
            for j in range(copies):
                o_ref[j, k] = piece

    many = pl.pallas_call(
        kernel,
        out_shape=jax.ShapeDtypeStruct((copies, n) + x.shape[1:], x.dtype),
        in_specs=[SM, VM],
        out_specs=VM,
        name="pick",
    )(index, x)
    return exchange(many, axes)


def tables(zh, c):
    half = HEAD // 2
    freq = jnp.exp(
        jnp.arange(half).astype(jnp.float32) * (-2.0 * math.log(500000.0) / HEAD)
    )
    t = zh * 1024 + jnp.arange(1024, dtype=jnp.int32)
    angles = t.astype(jnp.float32)[:, None] * freq[None, :]
    cos, sin = jnp.cos(angles), jnp.sin(angles)
    cos = jnp.concatenate([cos, cos], axis=1)
    sin = jnp.concatenate([-sin, sin], axis=1)
    is_key = c == 0
    return jnp.where(is_key, cos, 1.0), jnp.where(is_key, sin, 0.0)


def turn(place, mine, other, cos, sin):
    def kernel(p_ref, a_ref, b_ref, cos_ref, sin_ref, o_ref):
        for k in range(8):
            part = (a_ref if k < 4 else b_ref)[pl.ds(128 * (k % 4), 128), :]
            to = pl.ds(pl.multiple_of(p_ref[k] * 128, 128), 128)
            turned = part * cos_ref[to, :] + pltpu.roll(part, 64, 1) * sin_ref[to, :]
            o_ref[to, :] = turned.astype(jnp.bfloat16)

    return pl.pallas_call(
        kernel,
        out_shape=jax.ShapeDtypeStruct((1024, HEAD), jnp.bfloat16),
        in_specs=[SM] + [VM] * 4,
        out_specs=VM,
        name="turn",
    )(place, mine, other, cos, sin)


def attend_own(q, k, v):
    def kernel(q_ref, k_ref, v_ref, acc_ref, st_ref):
        for i in range(1024 // QB):
            rows = pl.ds(i * QB, QB)
            n = (i + 1) * QB
            r = lax.broadcasted_iota(jnp.int32, (QB, n), 0) + i * QB
            t = lax.broadcasted_iota(jnp.int32, (QB, n), 1)
            tops, totals = [], []
            for h in range(2):
                col = pl.ds(h * HEAD, HEAD)
                s = lax.dot_general(
                    q_ref[rows, col], k_ref[:n, :], NT, preferred_element_type=jnp.float32
                )
                s = jnp.where(t <= r, s, NEG)
                m = jnp.max(s, axis=1, keepdims=True)
                p = jnp.exp((s - m) * SCALE)
                tops.append(m)
                totals.append(jnp.sum(p, axis=1, keepdims=True))
                acc_ref[rows, col] = jnp.dot(
                    p.astype(jnp.bfloat16), v_ref[:n, :], preferred_element_type=jnp.float32
                )
            st_ref[rows, :] = jnp.concatenate(tops + totals, axis=1)

    return pl.pallas_call(
        kernel,
        out_shape=STATE,
        in_specs=[VM] * 3,
        out_specs=(VM,) * 2,
        name="attend_own",
    )(q, k, v)


def attend_more(who, q, first, partner, acc, st):
    part = 512

    def kernel(w_ref, q_ref, a_ref, b_ref, acc_ref, st_ref, o_ref, kv):
        @pl.when(pl.program_id(0) == 0)
        def _():
            kv[w_ref[1]] = a_ref[...]
            kv[1 - w_ref[1]] = b_ref[...]

        @pl.when(w_ref[0] == 0)
        def _():
            for h in range(2):
                col = pl.ds(h * HEAD, HEAD)
                o_ref[:, col] = (acc_ref[:, col] / st_ref[:, 2 + h : 3 + h]).astype(jnp.bfloat16)

        @pl.when(w_ref[0] != 0)
        def _():
            for h in range(2):
                col = pl.ds(h * HEAD, HEAD)
                tiles = [
                    lax.dot_general(
                        q_ref[:, col],
                        kv[0, t : t + part],
                        NT,
                        preferred_element_type=jnp.float32,
                    )
                    for t in range(0, 1024, part)
                ]
                m0 = st_ref[:, h : h + 1]
                m1 = m0
                for s in tiles:
                    m1 = jnp.maximum(m1, jnp.max(s, axis=1, keepdims=True))
                fade = jnp.exp2((m0 - m1) * SCALE2)
                total = st_ref[:, 2 + h : 3 + h] * fade
                out = acc_ref[:, col] * fade
                for t, s in enumerate(tiles):
                    p = jnp.exp2((s - m1) * SCALE2)
                    total = total + jnp.sum(p, axis=1, keepdims=True)
                    out = out + jnp.dot(
                        p.astype(jnp.bfloat16),
                        kv[1, t * part : (t + 1) * part],
                        preferred_element_type=jnp.float32,
                    )
                o_ref[:, col] = (out / total).astype(jnp.bfloat16)

    row = lambda width: pl.BlockSpec((QB, width), lambda i: (i, 0))
    whole = pl.BlockSpec((1024, HEAD), lambda i: (0, 0))
    return pl.pallas_call(
        kernel,
        grid=(1024 // QB,),
        out_shape=jax.ShapeDtypeStruct((1024, 256), jnp.bfloat16),
        in_specs=[SM, row(256), whole, whole, row(256), row(4)],
        out_specs=row(256),
        scratch_shapes=[pltpu.VMEM((2, 1024, HEAD), jnp.bfloat16)],
        name="attend_more",
    )(who, q, first, partner, acc, st)


def swap_cores(x):
    return lax.ppermute(x, "c", [(0, 1), (1, 0)])


def layer(queries, normed, key_weight_copies, value_weight_copies, owner):
    zh, x, c = lax.axis_index("zh"), lax.axis_index("x"), lax.axis_index("c")
    z_lo = lax.axis_index(("zf", "zn"))
    own_y, own_zf, own_zn = owner // 16, (owner // 4) % 4, owner % 4
    block8 = jnp.arange(8, dtype=jnp.int32)
    n = normed[0]

    w = jnp.stack([key_weight_copies[0], value_weight_copies[0]])
    w = w.reshape(2, 16, 8, 4, HEAD).transpose(3, 0, 1, 2, 4).reshape(128, 8, HEAD)
    w = exchange(w, ("x", "c", "y", "zn"))
    here = lax.dynamic_slice_in_dim(own_y * 4 + own_zn, zh * 8, 8)
    rows = [n]
    for s in (1, 2, 3):
        rows.append(lax.ppermute(n, "x", [(i, (i + s) % 4) for i in range(4)]))

    w = pick_spread(w, block8 * 16 + here, 8, ("zh", "zf"))
    block16 = jnp.arange(16, dtype=jnp.int32)
    index = ((block16 // 8) * 4 + own_zf) * 8 + block16 % 8
    w = pick_spread(w.reshape(64, 8, HEAD), index, 16, ("y", "zn"))
    w = w.transpose(1, 0, 2, 3).reshape(2048, HEAD)

    mine = jnp.concatenate(rows)
    other = swap_cores(mine)

    chip = (x - jnp.arange(4, dtype=jnp.int32)) % 4
    place = jnp.concatenate([chip * 2 + c, chip * 2 + 1 - c])
    cos, sin = tables(zh, c)
    raw = [jnp.dot(r, w, preferred_element_type=jnp.float32) for r in (mine, other)]
    kv = turn(place, *raw, cos, sin)

    up = lax.ppermute(kv, RING, [(i, i + 15) for i in range(8, 16)])
    down = lax.ppermute(kv, RING, [(i, i + 17) for i in range(8)])

    partner = swap_cores(kv)
    keys, values = jnp.where(c == 0, kv, partner), jnp.where(c == 0, partner, kv)
    q = queries[0].reshape(128, 8, 256).transpose(1, 0, 2)
    q = exchange(q, ("x", "c")).reshape(1024, 256)
    state = attend_own(q, keys, values)
    cache = exchange(kv.reshape(8, 128, HEAD), ("x", "c")).reshape(4, 2, 128, HEAD)
    cache_keys = cache[:, 0].transpose(1, 0, 2).reshape(1, 128, 512)
    cache_values = cache[:, 1].transpose(1, 0, 2).reshape(1, 128, 512)

    up, down, state, cache_keys, cache_values = lax.optimization_barrier(
        (up, down, state, cache_keys, cache_values)
    )
    up = lax.ppermute(up, RING, [(i, i + 1) for i in range(23, 31)])
    down = lax.ppermute(down, RING, [(i, i - 1) for i in range(17, 25)])
    first = jnp.where(z_lo >= 8, up, down)
    partner = swap_cores(first)
    state = attend_more(jnp.stack([zh, c]), q, first, partner, *state)
    out = exchange(state.reshape(8, 128, 256), ("x", "c"))
    attended = out.transpose(1, 0, 2).reshape(1, 128, 2048)
    return cache_keys, cache_values, attended


def solution(mesh):
    torus = Mesh(mesh.devices.reshape(2, 4, 2, 4, 4, 4), AXES)
    spec = P(("y", "zf", "zn"), ("zh", "x", "c"), None)
    return jax.shard_map(
        layer,
        mesh=torus,
        in_specs=(spec, spec, spec, spec, P()),
        out_specs=(spec, spec, spec),
        check_vma=False,
    )
```

```python
import math

import jax
import jax.numpy as jnp
from jax import lax
from jax.experimental import pallas as pl
from jax.experimental.pallas import tpu as pltpu
from jax.sharding import Mesh
from jax.sharding import PartitionSpec as P


HEAD = 128
SCALE = HEAD ** (-0.5)
SCALE2 = SCALE * math.log2(math.e)
NEG = -1e30
QB = 256
AXES = ("zh", "x", "c", "y", "zf", "zn")
RING = ("zh", "zf", "zn")
VM = pl.BlockSpec(memory_space=pltpu.VMEM)
SM = pl.BlockSpec(memory_space=pltpu.SMEM)
NT = (((1,), (1,)), ((), ()))
STATE = (
    jax.ShapeDtypeStruct((1024, 256), jnp.float32),
    jax.ShapeDtypeStruct((1024, 4), jnp.float32),
)


def exchange(x, axes):
    return lax.all_to_all(x, axes, 0, 0, tiled=True)


def pick_spread(x, index, copies, axes):
    n = index.shape[0]

    def kernel(i_ref, x_ref, o_ref):
        for k in range(n):
            piece = x_ref[i_ref[k]]
            for j in range(copies):
                o_ref[j, k] = piece

    many = pl.pallas_call(
        kernel,
        out_shape=jax.ShapeDtypeStruct((copies, n) + x.shape[1:], x.dtype),
        in_specs=[SM, VM],
        out_specs=VM,
        name="pick",
    )(index, x)
    return exchange(many, axes)


def tables(zh, c):
    half = HEAD // 2
    freq = jnp.exp(
        jnp.arange(half).astype(jnp.float32) * (-2.0 * math.log(500000.0) / HEAD)
    )
    t = zh * 1024 + jnp.arange(1024, dtype=jnp.int32)
    angles = t.astype(jnp.float32)[:, None] * freq[None, :]
    cos, sin = jnp.cos(angles), jnp.sin(angles)
    cos = jnp.concatenate([cos, cos], axis=1)
    sin = jnp.concatenate([-sin, sin], axis=1)
    is_key = c == 0
    return jnp.where(is_key, cos, 1.0), jnp.where(is_key, sin, 0.0)


def turn(place, mine, other, cos, sin):
    def kernel(p_ref, a_ref, b_ref, cos_ref, sin_ref, o_ref):
        for k in range(8):
            part = (a_ref if k < 4 else b_ref)[pl.ds(128 * (k % 4), 128), :]
            to = pl.ds(pl.multiple_of(p_ref[k] * 128, 128), 128)
            turned = part * cos_ref[to, :] + pltpu.roll(part, 64, 1) * sin_ref[to, :]
            o_ref[to, :] = turned.astype(jnp.bfloat16)

    return pl.pallas_call(
        kernel,
        out_shape=jax.ShapeDtypeStruct((1024, HEAD), jnp.bfloat16),
        in_specs=[SM] + [VM] * 4,
        out_specs=VM,
        name="turn",
    )(place, mine, other, cos, sin)


def attend_own(q, k, v):
    def kernel(q_ref, k_ref, v_ref, acc_ref, st_ref):
        for i in range(1024 // QB):
            rows = pl.ds(i * QB, QB)
            n = (i + 1) * QB
            r = lax.broadcasted_iota(jnp.int32, (QB, n), 0) + i * QB
            t = lax.broadcasted_iota(jnp.int32, (QB, n), 1)
            tops, totals = [], []
            for h in range(2):
                col = pl.ds(h * HEAD, HEAD)
                s = lax.dot_general(
                    q_ref[rows, col], k_ref[:n, :], NT, preferred_element_type=jnp.float32
                )
                s = jnp.where(t <= r, s, NEG)
                m = jnp.max(s, axis=1, keepdims=True)
                p = jnp.exp((s - m) * SCALE)
                tops.append(m)
                totals.append(jnp.sum(p, axis=1, keepdims=True))
                acc_ref[rows, col] = jnp.dot(
                    p.astype(jnp.bfloat16), v_ref[:n, :], preferred_element_type=jnp.float32
                )
            st_ref[rows, :] = jnp.concatenate(tops + totals, axis=1)

    return pl.pallas_call(
        kernel,
        out_shape=STATE,
        in_specs=[VM] * 3,
        out_specs=(VM,) * 2,
        name="attend_own",
    )(q, k, v)


def attend_more(who, q, first, partner, acc, st):
    part = 512

    def kernel(w_ref, q_ref, a_ref, b_ref, acc_ref, st_ref, o_ref, kv):
        @pl.when(pl.program_id(0) == 0)
        def _():
            kv[w_ref[1]] = a_ref[...]
            kv[1 - w_ref[1]] = b_ref[...]

        @pl.when(w_ref[0] == 0)
        def _():
            for h in range(2):
                col = pl.ds(h * HEAD, HEAD)
                o_ref[:, col] = (acc_ref[:, col] / st_ref[:, 2 + h : 3 + h]).astype(jnp.bfloat16)

        @pl.when(w_ref[0] != 0)
        def _():
            for h in range(2):
                col = pl.ds(h * HEAD, HEAD)
                tiles = [
                    lax.dot_general(
                        q_ref[:, col],
                        kv[0, t : t + part],
                        NT,
                        preferred_element_type=jnp.float32,
                    )
                    for t in range(0, 1024, part)
                ]
                m0 = st_ref[:, h : h + 1]
                m1 = m0
                for s in tiles:
                    m1 = jnp.maximum(m1, jnp.max(s, axis=1, keepdims=True))
                fade = jnp.exp2((m0 - m1) * SCALE2)
                total = st_ref[:, 2 + h : 3 + h] * fade
                out = acc_ref[:, col] * fade
                for t, s in enumerate(tiles):
                    p = jnp.exp2((s - m1) * SCALE2)
                    total = total + jnp.sum(p, axis=1, keepdims=True)
                    out = out + jnp.dot(
                        p.astype(jnp.bfloat16),
                        kv[1, t * part : (t + 1) * part],
                        preferred_element_type=jnp.float32,
                    )
                o_ref[:, col] = (out / total).astype(jnp.bfloat16)

    row = lambda width: pl.BlockSpec((QB, width), lambda i: (i, 0))
    whole = pl.BlockSpec((1024, HEAD), lambda i: (0, 0))
    return pl.pallas_call(
        kernel,
        grid=(1024 // QB,),
        out_shape=jax.ShapeDtypeStruct((1024, 256), jnp.bfloat16),
        in_specs=[SM, row(256), whole, whole, row(256), row(4)],
        out_specs=row(256),
        scratch_shapes=[pltpu.VMEM((2, 1024, HEAD), jnp.bfloat16)],
        name="attend_more",
    )(who, q, first, partner, acc, st)


def swap_cores(x):
    return lax.ppermute(x, "c", [(0, 1), (1, 0)])


def layer(queries, normed, key_weight_copies, value_weight_copies, owner):
    zh, x, c = lax.axis_index("zh"), lax.axis_index("x"), lax.axis_index("c")
    own_y, own_zf, own_zn = owner // 16, (owner // 4) % 4, owner % 4
    block8 = jnp.arange(8, dtype=jnp.int32)
    n = normed[0]

    w = jnp.stack([key_weight_copies[0], value_weight_copies[0]])
    w = w.reshape(2, 16, 8, 4, HEAD).transpose(3, 0, 1, 2, 4).reshape(128, 8, HEAD)
    w = exchange(w, ("x", "c", "y", "zn"))
    here = lax.dynamic_slice_in_dim(own_y * 4 + own_zn, zh * 8, 8)
    rows = [n]
    for s in (1, 2, 3):
        rows.append(lax.ppermute(n, "x", [(i, (i + s) % 4) for i in range(4)]))

    w = pick_spread(w, block8 * 16 + here, 8, ("zh", "zf"))
    block16 = jnp.arange(16, dtype=jnp.int32)
    index = ((block16 // 8) * 4 + own_zf) * 8 + block16 % 8
    w = pick_spread(w.reshape(64, 8, HEAD), index, 16, ("y", "zn"))
    w = w.transpose(1, 0, 2, 3).reshape(2048, HEAD)

    mine = jnp.concatenate(rows)
    other = swap_cores(mine)

    chip = (x - jnp.arange(4, dtype=jnp.int32)) % 4
    place = jnp.concatenate([chip * 2 + c, chip * 2 + 1 - c])
    cos, sin = tables(zh, c)
    raw = [jnp.dot(r, w, preferred_element_type=jnp.float32) for r in (mine, other)]
    kv = turn(place, *raw, cos, sin)

    first = lax.ppermute(kv, RING, [(i, i + 16) for i in range(16)])

    partner = swap_cores(kv)
    keys, values = jnp.where(c == 0, kv, partner), jnp.where(c == 0, partner, kv)
    q = queries[0].reshape(128, 8, 256).transpose(1, 0, 2)
    q = exchange(q, ("x", "c")).reshape(1024, 256)
    state = attend_own(q, keys, values)
    cache = exchange(kv.reshape(8, 128, HEAD), ("x", "c")).reshape(4, 2, 128, HEAD)
    cache_keys = cache[:, 0].transpose(1, 0, 2).reshape(1, 128, 512)
    cache_values = cache[:, 1].transpose(1, 0, 2).reshape(1, 128, 512)

    first, state, cache_keys, cache_values = lax.optimization_barrier(
        (first, state, cache_keys, cache_values)
    )
    partner = swap_cores(first)
    state = attend_more(jnp.stack([zh, c]), q, first, partner, *state)
    out = exchange(state.reshape(8, 128, 256), ("x", "c"))
    attended = out.transpose(1, 0, 2).reshape(1, 128, 2048)
    return cache_keys, cache_values, attended


def solution(mesh):
    torus = Mesh(mesh.devices.reshape(2, 4, 2, 4, 4, 4), AXES)
    spec = P(("y", "zf", "zn"), ("zh", "x", "c"), None)
    return jax.shard_map(
        layer,
        mesh=torus,
        in_specs=(spec, spec, spec, spec, P()),
        out_specs=(spec, spec, spec),
        check_vma=False,
    )
```

```python
import math

import jax
import jax.numpy as jnp
from jax import lax
from jax.experimental import pallas as pl
from jax.experimental.pallas import tpu as pltpu
from jax.sharding import Mesh
from jax.sharding import PartitionSpec as P


HEAD = 128
SCALE = HEAD ** (-0.5)
SCALE2 = SCALE * math.log2(math.e)
NEG = -1e30
QB = 256
AXES = ("zh", "x", "c", "y", "zf", "zn")
RING = ("zh", "zf", "zn")
VM = pl.BlockSpec(memory_space=pltpu.VMEM)
SM = pl.BlockSpec(memory_space=pltpu.SMEM)
NT = (((1,), (1,)), ((), ()))
STATE = (
    jax.ShapeDtypeStruct((1024, 256), jnp.float32),
    jax.ShapeDtypeStruct((1024, 4), jnp.float32),
)


def exchange(x, axes):
    return lax.all_to_all(x, axes, 0, 0, tiled=True)


def pick_spread(x, index, copies, axes):
    n = index.shape[0]

    def kernel(i_ref, x_ref, o_ref):
        for k in range(n):
            piece = x_ref[i_ref[k]]
            for j in range(copies):
                o_ref[j, k] = piece

    many = pl.pallas_call(
        kernel,
        out_shape=jax.ShapeDtypeStruct((copies, n) + x.shape[1:], x.dtype),
        in_specs=[SM, VM],
        out_specs=VM,
        name="pick",
    )(index, x)
    return exchange(many, axes)


def tables(zh, c):
    half = HEAD // 2
    freq = jnp.exp(
        jnp.arange(half).astype(jnp.float32) * (-2.0 * math.log(500000.0) / HEAD)
    )
    t = zh * 1024 + jnp.arange(1024, dtype=jnp.int32)
    angles = t.astype(jnp.float32)[:, None] * freq[None, :]
    cos, sin = jnp.cos(angles), jnp.sin(angles)
    cos = jnp.concatenate([cos, cos], axis=1)
    sin = jnp.concatenate([-sin, sin], axis=1)
    is_key = c == 0
    return jnp.where(is_key, cos, 1.0), jnp.where(is_key, sin, 0.0)


def project(run, place, mine, other, w, cos, sin, before=None):
    def kernel(p_ref, a0, a1, a2, a3, b_ref, w_ref, cos_ref, sin_ref, *rest):
        old, (o_ref, rows, wv, cv, sv, sems) = rest[:-6], rest[-6:]

        @pl.when(p_ref[8] == 1)
        def _():
            pairs = [(w_ref, wv), (cos_ref, cv), (sin_ref, sv)]
            pairs += [(a, rows.at[k]) for k, a in enumerate((a0, a1, a2, a3))]
            pairs += [(b_ref.at[pl.ds(128 * k, 128)], rows.at[4 + k]) for k in range(4)]
            copies = [pltpu.make_async_copy(s, d, sems.at[k]) for k, (s, d) in enumerate(pairs)]
            for copy in copies:
                copy.start()
            for copy in copies[:3]:
                copy.wait()
            for k in range(8):
                copies[3 + k].wait()
                raw = jnp.dot(rows[k], wv[...], preferred_element_type=jnp.float32)
                to = pl.ds(pl.multiple_of(p_ref[k] * 128, 128), 128)
                turned = raw * cv[to, :] + pltpu.roll(raw, 64, 1) * sv[to, :]
                o_ref[to, :] = turned.astype(jnp.bfloat16)

        @pl.when(p_ref[8] != 1)
        def _():
            if old:
                copy = pltpu.make_async_copy(old[0], o_ref, sems.at[0])
                copy.start()
                copy.wait()
            else:
                o_ref[...] = jnp.zeros_like(o_ref)

    extra = () if before is None else (before,)
    return pl.pallas_call(
        kernel,
        out_shape=jax.ShapeDtypeStruct((1024, HEAD), jnp.bfloat16),
        in_specs=[SM] + [pl.BlockSpec(memory_space=pl.ANY)] * (8 + len(extra)),
        out_specs=VM,
        scratch_shapes=[
            pltpu.VMEM((8, 128, 2048), jnp.bfloat16),
            pltpu.VMEM((2048, HEAD), jnp.bfloat16),
            pltpu.VMEM((1024, HEAD), jnp.float32),
            pltpu.VMEM((1024, HEAD), jnp.float32),
            pltpu.SemaphoreType.DMA((11,)),
        ],
        name="project",
    )(jnp.concatenate([place, run.reshape(1)]), *mine, other, w, cos, sin, *extra)


def attend_own(q, k, v):
    def kernel(q_ref, k_ref, v_ref, acc_ref, st_ref):
        for i in range(1024 // QB):
            rows = pl.ds(i * QB, QB)
            n = (i + 1) * QB
            r = lax.broadcasted_iota(jnp.int32, (QB, n), 0) + i * QB
            t = lax.broadcasted_iota(jnp.int32, (QB, n), 1)
            tops, totals = [], []
            for h in range(2):
                col = pl.ds(h * HEAD, HEAD)
                s = lax.dot_general(
                    q_ref[rows, col], k_ref[:n, :], NT, preferred_element_type=jnp.float32
                )
                s = jnp.where(t <= r, s, NEG)
                m = jnp.max(s, axis=1, keepdims=True)
                p = jnp.exp((s - m) * SCALE)
                tops.append(m)
                totals.append(jnp.sum(p, axis=1, keepdims=True))
                acc_ref[rows, col] = jnp.dot(
                    p.astype(jnp.bfloat16), v_ref[:n, :], preferred_element_type=jnp.float32
                )
            st_ref[rows, :] = jnp.concatenate(tops + totals, axis=1)

    return pl.pallas_call(
        kernel,
        out_shape=STATE,
        in_specs=[VM] * 3,
        out_specs=(VM,) * 2,
        name="attend_own",
    )(q, k, v)


def attend_more(who, q, first, partner, acc, st):
    part = 512

    def kernel(w_ref, q_ref, a_ref, b_ref, acc_ref, st_ref, o_ref, kv):
        @pl.when(pl.program_id(0) == 0)
        def _():
            kv[w_ref[1]] = a_ref[...]
            kv[1 - w_ref[1]] = b_ref[...]

        @pl.when(w_ref[0] == 0)
        def _():
            for h in range(2):
                col = pl.ds(h * HEAD, HEAD)
                o_ref[:, col] = (acc_ref[:, col] / st_ref[:, 2 + h : 3 + h]).astype(jnp.bfloat16)

        @pl.when(w_ref[0] != 0)
        def _():
            for h in range(2):
                col = pl.ds(h * HEAD, HEAD)
                tiles = [
                    lax.dot_general(
                        q_ref[:, col],
                        kv[0, t : t + part],
                        NT,
                        preferred_element_type=jnp.float32,
                    )
                    for t in range(0, 1024, part)
                ]
                m0 = st_ref[:, h : h + 1]
                m1 = m0
                for s in tiles:
                    m1 = jnp.maximum(m1, jnp.max(s, axis=1, keepdims=True))
                fade = jnp.exp2((m0 - m1) * SCALE2)
                total = st_ref[:, 2 + h : 3 + h] * fade
                out = acc_ref[:, col] * fade
                for t, s in enumerate(tiles):
                    p = jnp.exp2((s - m1) * SCALE2)
                    total = total + jnp.sum(p, axis=1, keepdims=True)
                    out = out + jnp.dot(
                        p.astype(jnp.bfloat16),
                        kv[1, t * part : (t + 1) * part],
                        preferred_element_type=jnp.float32,
                    )
                o_ref[:, col] = (out / total).astype(jnp.bfloat16)

    row = lambda width: pl.BlockSpec((QB, width), lambda i: (i, 0))
    whole = pl.BlockSpec((1024, HEAD), lambda i: (0, 0))
    return pl.pallas_call(
        kernel,
        grid=(1024 // QB,),
        out_shape=jax.ShapeDtypeStruct((1024, 256), jnp.bfloat16),
        in_specs=[SM, row(256), whole, whole, row(256), row(4)],
        out_specs=row(256),
        scratch_shapes=[pltpu.VMEM((2, 1024, HEAD), jnp.bfloat16)],
        name="attend_more",
    )(who, q, first, partner, acc, st)


def swap_cores(x):
    return lax.ppermute(x, "c", [(0, 1), (1, 0)])


def layer(queries, normed, key_weight_copies, value_weight_copies, owner):
    zh, x, c = lax.axis_index("zh"), lax.axis_index("x"), lax.axis_index("c")
    own_y, own_zf, own_zn = owner // 16, (owner // 4) % 4, owner % 4
    block8 = jnp.arange(8, dtype=jnp.int32)
    n = normed[0]

    w = jnp.stack([key_weight_copies[0], value_weight_copies[0]])
    w = w.reshape(2, 16, 8, 4, HEAD).transpose(3, 0, 1, 2, 4).reshape(128, 8, HEAD)
    w = exchange(w, ("x", "c", "y", "zn"))
    here = lax.dynamic_slice_in_dim(own_y * 4 + own_zn, zh * 8, 8)
    rows = [n]
    for s in (1, 2, 3):
        rows.append(lax.ppermute(n, "x", [(i, (i + s) % 4) for i in range(4)]))

    w = pick_spread(w, block8 * 16 + here, 8, ("zh", "zf"))
    block16 = jnp.arange(16, dtype=jnp.int32)
    index = ((block16 // 8) * 4 + own_zf) * 8 + block16 % 8
    w = pick_spread(w.reshape(64, 8, HEAD), index, 16, ("y", "zn"))
    w = w.transpose(1, 0, 2, 3).reshape(2048, HEAD)

    other = swap_cores(jnp.concatenate(rows))

    chip = (x - jnp.arange(4, dtype=jnp.int32)) % 4
    place = jnp.concatenate([chip * 2 + c, chip * 2 + 1 - c])
    other, half = lax.optimization_barrier((other, zh))
    cos, sin = tables(half, c)
    parts = (place, rows, other, w, cos, sin)

    sent = project(1 - zh, *parts)
    first = lax.ppermute(sent, RING, [(i, i + 16) for i in range(16)])

    kv = project(zh, *parts, sent)
    partner = swap_cores(kv)
    keys, values = jnp.where(c == 0, kv, partner), jnp.where(c == 0, partner, kv)
    q = queries[0].reshape(128, 8, 256).transpose(1, 0, 2)
    q = exchange(q, ("x", "c")).reshape(1024, 256)
    state = attend_own(q, keys, values)
    cache = exchange(kv.reshape(8, 128, HEAD), ("x", "c")).reshape(4, 2, 128, HEAD)
    cache_keys = cache[:, 0].transpose(1, 0, 2).reshape(1, 128, 512)
    cache_values = cache[:, 1].transpose(1, 0, 2).reshape(1, 128, 512)

    first, state, cache_keys, cache_values = lax.optimization_barrier(
        (first, state, cache_keys, cache_values)
    )
    partner = swap_cores(first)
    state = attend_more(jnp.stack([zh, c]), q, first, partner, *state)
    out = exchange(state.reshape(8, 128, 256), ("x", "c"))
    attended = out.transpose(1, 0, 2).reshape(1, 128, 2048)
    return cache_keys, cache_values, attended


def solution(mesh):
    torus = Mesh(mesh.devices.reshape(2, 4, 2, 4, 4, 4), AXES)
    spec = P(("y", "zf", "zn"), ("zh", "x", "c"), None)
    return jax.shard_map(
        layer,
        mesh=torus,
        in_specs=(spec, spec, spec, spec, P()),
        out_specs=(spec, spec, spec),
        check_vma=False,
    )
```

```python
import math

import jax
import jax.numpy as jnp
from jax import lax
from jax.experimental import pallas as pl
from jax.experimental.pallas import tpu as pltpu
from jax.sharding import Mesh
from jax.sharding import PartitionSpec as P


HEAD = 128
SCALE = HEAD ** (-0.5)
SCALE2 = SCALE * math.log2(math.e)
NEG = -1e30
QB = 256
AXES = ("zh", "x", "c", "y", "zf", "zn")
RING = ("zh", "zf", "zn")
VM = pl.BlockSpec(memory_space=pltpu.VMEM)
SM = pl.BlockSpec(memory_space=pltpu.SMEM)
NT = (((1,), (1,)), ((), ()))
STATE = (
    jax.ShapeDtypeStruct((1024, 256), jnp.float32),
    jax.ShapeDtypeStruct((1024, 4), jnp.float32),
)


def exchange(x, axes):
    return lax.all_to_all(x, axes, 0, 0, tiled=True)


def pick_spread(x, index, copies, axes):
    n = index.shape[0]

    def kernel(i_ref, x_ref, o_ref):
        for k in range(n):
            piece = x_ref[i_ref[k]]
            for j in range(copies):
                o_ref[j, k] = piece

    many = pl.pallas_call(
        kernel,
        out_shape=jax.ShapeDtypeStruct((copies, n) + x.shape[1:], x.dtype),
        in_specs=[SM, VM],
        out_specs=VM,
        name="pick",
    )(index, x)
    return exchange(many, axes)


def tables(zh, c):
    half = HEAD // 2
    freq = jnp.exp(
        jnp.arange(half).astype(jnp.float32) * (-2.0 * math.log(500000.0) / HEAD)
    )
    t = zh * 1024 + jnp.arange(1024, dtype=jnp.int32)
    angles = t.astype(jnp.float32)[:, None] * freq[None, :]
    cos, sin = jnp.cos(angles), jnp.sin(angles)
    cos = jnp.concatenate([cos, cos], axis=1)
    sin = jnp.concatenate([-sin, sin], axis=1)
    is_key = c == 0
    return jnp.where(is_key, cos, 1.0), jnp.where(is_key, sin, 0.0)


def project(run, place, mine, other, w, cos, sin, before=None):
    def kernel(p_ref, a0, a1, a2, a3, b_ref, w_ref, cos_ref, sin_ref, *rest):
        old, (o_ref, rows, wv, cv, sv, sems) = rest[:-6], rest[-6:]

        @pl.when(p_ref[8] == 1)
        def _():
            pairs = [(w_ref, wv), (cos_ref, cv), (sin_ref, sv)]
            pairs += [(a, rows.at[k]) for k, a in enumerate((a0, a1, a2, a3))]
            pairs += [(b_ref.at[pl.ds(128 * k, 128)], rows.at[4 + k]) for k in range(4)]
            copies = [pltpu.make_async_copy(s, d, sems.at[k]) for k, (s, d) in enumerate(pairs)]
            for copy in copies:
                copy.start()
            for copy in copies[:3]:
                copy.wait()
            for k in range(8):
                copies[3 + k].wait()
                raw = jnp.dot(rows[k], wv[...], preferred_element_type=jnp.float32)
                to = pl.ds(pl.multiple_of(p_ref[k] * 128, 128), 128)
                turned = raw * cv[to, :] + pltpu.roll(raw, 64, 1) * sv[to, :]
                o_ref[to, :] = turned.astype(jnp.bfloat16)

        @pl.when(p_ref[8] != 1)
        def _():
            if old:
                copy = pltpu.make_async_copy(old[0], o_ref, sems.at[0])
                copy.start()
                copy.wait()
            else:
                o_ref[...] = jnp.zeros_like(o_ref)

    extra = () if before is None else (before,)
    return pl.pallas_call(
        kernel,
        out_shape=jax.ShapeDtypeStruct((1024, HEAD), jnp.bfloat16),
        in_specs=[SM] + [pl.BlockSpec(memory_space=pl.ANY)] * (8 + len(extra)),
        out_specs=VM,
        scratch_shapes=[
            pltpu.VMEM((8, 128, 2048), jnp.bfloat16),
            pltpu.VMEM((2048, HEAD), jnp.bfloat16),
            pltpu.VMEM((1024, HEAD), jnp.float32),
            pltpu.VMEM((1024, HEAD), jnp.float32),
            pltpu.SemaphoreType.DMA((11,)),
        ],
        name="project",
    )(jnp.concatenate([place, run.reshape(1)]), *mine, other, w, cos, sin, *extra)


def attend_own(q, k, v):
    def kernel(q_ref, k_ref, v_ref, acc_ref, st_ref):
        for i in range(1024 // QB):
            rows = pl.ds(i * QB, QB)
            n = (i + 1) * QB
            r = lax.broadcasted_iota(jnp.int32, (QB, n), 0) + i * QB
            t = lax.broadcasted_iota(jnp.int32, (QB, n), 1)
            tops, totals = [], []
            for h in range(2):
                col = pl.ds(h * HEAD, HEAD)
                s = lax.dot_general(
                    q_ref[rows, col], k_ref[:n, :], NT, preferred_element_type=jnp.float32
                )
                s = jnp.where(t <= r, s, NEG)
                m = jnp.max(s, axis=1, keepdims=True)
                p = jnp.exp((s - m) * SCALE)
                tops.append(m)
                totals.append(jnp.sum(p, axis=1, keepdims=True))
                acc_ref[rows, col] = jnp.dot(
                    p.astype(jnp.bfloat16), v_ref[:n, :], preferred_element_type=jnp.float32
                )
            st_ref[rows, :] = jnp.concatenate(tops + totals, axis=1)

    return pl.pallas_call(
        kernel,
        out_shape=STATE,
        in_specs=[VM] * 3,
        out_specs=(VM,) * 2,
        name="attend_own",
    )(q, k, v)


def attend_more(h, who, q, first, partner, acc, st):
    part = 512

    def kernel(w_ref, q_ref, a_ref, b_ref, acc_ref, st_ref, o_ref, kv):
        @pl.when(pl.program_id(0) == 0)
        def _():
            kv[w_ref[1]] = a_ref[...]
            kv[1 - w_ref[1]] = b_ref[...]

        @pl.when(w_ref[0] == 0)
        def _():
            o_ref[...] = (acc_ref[...] / st_ref[:, 2 + h : 3 + h]).astype(jnp.bfloat16)

        @pl.when(w_ref[0] != 0)
        def _():
            tiles = [
                lax.dot_general(
                    q_ref[...],
                    kv[0, t : t + part],
                    NT,
                    preferred_element_type=jnp.float32,
                )
                for t in range(0, 1024, part)
            ]
            m0 = st_ref[:, h : h + 1]
            m1 = m0
            for s in tiles:
                m1 = jnp.maximum(m1, jnp.max(s, axis=1, keepdims=True))
            fade = jnp.exp2((m0 - m1) * SCALE2)
            total = st_ref[:, 2 + h : 3 + h] * fade
            out = acc_ref[...] * fade
            for t, s in enumerate(tiles):
                p = jnp.exp2((s - m1) * SCALE2)
                total = total + jnp.sum(p, axis=1, keepdims=True)
                out = out + jnp.dot(
                    p.astype(jnp.bfloat16),
                    kv[1, t * part : (t + 1) * part],
                    preferred_element_type=jnp.float32,
                )
            o_ref[...] = (out / total).astype(jnp.bfloat16)

    head = pl.BlockSpec((QB, HEAD), lambda i: (i, h))
    row = lambda width: pl.BlockSpec((QB, width), lambda i: (i, 0))
    whole = pl.BlockSpec((1024, HEAD), lambda i: (0, 0))
    return pl.pallas_call(
        kernel,
        grid=(1024 // QB,),
        out_shape=jax.ShapeDtypeStruct((1024, HEAD), jnp.bfloat16),
        in_specs=[SM, head, whole, whole, head, row(4)],
        out_specs=row(HEAD),
        scratch_shapes=[pltpu.VMEM((2, 1024, HEAD), jnp.bfloat16)],
        name="attend_more",
    )(who, q, first, partner, acc, st)


def swap_cores(x):
    return lax.ppermute(x, "c", [(0, 1), (1, 0)])


def layer(queries, normed, key_weight_copies, value_weight_copies, owner):
    zh, x, c = lax.axis_index("zh"), lax.axis_index("x"), lax.axis_index("c")
    own_y, own_zf, own_zn = owner // 16, (owner // 4) % 4, owner % 4
    block8 = jnp.arange(8, dtype=jnp.int32)
    n = normed[0]

    w = jnp.stack([key_weight_copies[0], value_weight_copies[0]])
    w = w.reshape(2, 16, 8, 4, HEAD).transpose(3, 0, 1, 2, 4).reshape(128, 8, HEAD)
    w = exchange(w, ("x", "c", "y", "zn"))
    here = lax.dynamic_slice_in_dim(own_y * 4 + own_zn, zh * 8, 8)
    rows = [n]
    for s in (1, 2, 3):
        rows.append(lax.ppermute(n, "x", [(i, (i + s) % 4) for i in range(4)]))

    w = pick_spread(w, block8 * 16 + here, 8, ("zh", "zf"))
    block16 = jnp.arange(16, dtype=jnp.int32)
    index = ((block16 // 8) * 4 + own_zf) * 8 + block16 % 8
    w = pick_spread(w.reshape(64, 8, HEAD), index, 16, ("y", "zn"))
    w = w.transpose(1, 0, 2, 3).reshape(2048, HEAD)

    other = swap_cores(jnp.concatenate(rows))

    chip = (x - jnp.arange(4, dtype=jnp.int32)) % 4
    place = jnp.concatenate([chip * 2 + c, chip * 2 + 1 - c])
    other, half = lax.optimization_barrier((other, zh))
    cos, sin = tables(half, c)
    parts = (place, rows, other, w, cos, sin)

    sent = project(1 - zh, *parts)
    first = lax.ppermute(sent, RING, [(i, i + 16) for i in range(16)])

    kv = project(zh, *parts, sent)
    partner = swap_cores(kv)
    keys, values = jnp.where(c == 0, kv, partner), jnp.where(c == 0, partner, kv)
    q = queries[0].reshape(128, 8, 256).transpose(1, 0, 2)
    q = exchange(q, ("x", "c")).reshape(1024, 256)
    state = attend_own(q, keys, values)
    cache = exchange(kv.reshape(8, 128, HEAD), ("x", "c")).reshape(4, 2, 128, HEAD)
    cache_keys = cache[:, 0].transpose(1, 0, 2).reshape(1, 128, 512)
    cache_values = cache[:, 1].transpose(1, 0, 2).reshape(1, 128, 512)

    first, state, cache_keys, cache_values = lax.optimization_barrier(
        (first, state, cache_keys, cache_values)
    )
    partner = swap_cores(first)
    outs = []
    for h in range(2):
        out = attend_more(h, jnp.stack([zh, c]), q, first, partner, *state)
        outs.append(exchange(out.reshape(8, 128, HEAD), ("x", "c")))
    out = jnp.concatenate(outs, axis=1).reshape(16, 128, HEAD)
    attended = out.transpose(1, 0, 2).reshape(1, 128, 2048)
    return cache_keys, cache_values, attended


def solution(mesh):
    torus = Mesh(mesh.devices.reshape(2, 4, 2, 4, 4, 4), AXES)
    spec = P(("y", "zf", "zn"), ("zh", "x", "c"), None)
    return jax.shard_map(
        layer,
        mesh=torus,
        in_specs=(spec, spec, spec, spec, P()),
        out_specs=(spec, spec, spec),
        check_vma=False,
    )
```
